32 devices in a mesh: dop: 8 (over z, y), slow: 4 (over x, core).
Axes of the slice: x: 2, y: 2, z: 4, core: 2. Of those that a mesh axis runs over, the one named last changes fastest.
Arguments:
- profiles: bfloat16 [32, 2, 1024, 2048], P('slow', None, 'dop'), may hold values from -6 to 6
- range_walk: int32 [2048], replicated, may hold values from -32 to 32
- band_order: int32 [32], replicated, may hold values from 0 to 31, each once
Outputs:
- ambiguity: float32 [2048, 1024], P(('dop', 'slow'))
The draws below stay inside these ranges and needn't reach their ends.
Inputs may be any that keep to these rules, and one draw needn't show every extreme that they name: `band_order`: each band number appears exactly once.
All inputs are finite; a program needn't handle non-finite values.
Results may differ from the reference program's by a relative error of at most 0.00067.
Values sent between devices are 32-bit elements; how exact they have to be, the bound alone decides.
A program may use at most 128 MiB of HBM per device.

```python
import math
import jax
import jax.numpy as jnp
from jax import lax

F = 2048
R = 1024
WALK = 32
BATCHES = 32
BANDS = 32
BAND_ROWS = 64


def plant(result, own_key, smallest, top_value):
    dims = result.shape
    index_at = [jax.random.randint(jax.random.fold_in(own_key, axis), (), 0, dims[axis]) for axis in range(len(dims))]
    result = result.at[tuple(index_at)].set(smallest)
    longest = dims.index(max(dims))
    index_at[longest] = (index_at[longest] + 1) % dims[longest]
    return result.at[tuple(index_at)].set(top_value)


def steps_of(own_key, shape, cuts, least, top_value):
    factor_of = 1.0
    for axis_at, blocks in cuts:
        heights = jax.random.uniform(jax.random.fold_in(jax.random.fold_in(own_key, 6), axis_at), (blocks,), jnp.float32, least / len(cuts), top_value / len(cuts))
        factor_of = factor_of * jnp.repeat(jnp.exp(heights), shape[axis_at] // blocks).reshape((-1,) + (1,) * (len(shape) - 1 - axis_at))
    return factor_of


def bell_draw(key, extent, deviation, bound, split=(), held_as=jnp.bfloat16):
    drawn = deviation * jax.random.normal(key, extent, jnp.float32)
    if split:
        drawn = drawn * steps_of(key, extent, split, -0.22, 0.18)
    return jnp.clip(drawn, -bound, bound).astype(held_as)


def setup_inputs(seed: int = 0) -> dict:
    streams_of = jax.random.split(jax.random.key(seed), 4)
    profiles = bell_draw(streams_of[0], (BATCHES, 2, R, F), 1.0, 6.0, ((0, 4), (2, 8)))
    range_walk = plant(jax.random.randint(streams_of[1], (F,), -WALK, WALK + 1), jax.random.fold_in(streams_of[1], 1), -WALK, WALK).astype(jnp.int32)
    band_order = jax.random.permutation(streams_of[2], BANDS).astype(jnp.int32)
    return dict(profiles=profiles, range_walk=range_walk, band_order=band_order)


def fourier_tables(length):
    counter = jnp.arange(length, dtype=jnp.int32)
    phases = (counter[:, None] * counter[None, :]) % length
    angles = phases.astype(jnp.float32) * (2.0 * math.pi / length)
    return jnp.cos(angles).astype(jnp.bfloat16), jnp.sin(angles).astype(jnp.bfloat16)


def batch_powers(block, cosine, sine_table):
    count = block.shape[0]
    delays = block.shape[2]
    bins = block.shape[3]
    stacked = block.reshape(count * 2 * delays, bins)
    first = jnp.dot(stacked, cosine, preferred_element_type=jnp.float32).reshape(count, 2, delays, bins)
    second = jnp.dot(stacked, sine_table, preferred_element_type=jnp.float32).reshape(count, 2, delays, bins)
    real_part = first[:, 0] + second[:, 1]
    imag_part = first[:, 1] - second[:, 0]
    return real_part * real_part + imag_part * imag_part


def reference(profiles, range_walk, band_order):
    cosine, sine_table = fourier_tables(F)

    def accumulate(running, inputs):
        block, batch = inputs
        powers = batch_powers(block[None], cosine, sine_table)[0]
        offsets = (range_walk * batch) // BATCHES
        padded = jnp.pad(powers, ((WALK, WALK), (0, 0)))
        lookup = jnp.arange(R, dtype=jnp.int32)[:, None] + offsets[None, :] + WALK
        aligned = jnp.take_along_axis(padded, lookup.astype(jnp.int32), axis=0)
        return running + aligned, jnp.zeros((), jnp.float32)

    start = jnp.zeros((R, F), jnp.float32)
    scanned = lax.scan(accumulate, start, (profiles, jnp.arange(BATCHES, dtype=jnp.int32)))
    power_map = (scanned[0] * (1.0 / (BATCHES * F))).T
    ordered = jnp.take(power_map.reshape(BANDS, BAND_ROWS, R), band_order, axis=0)
    return ordered.reshape(F, R)
```

```python
import functools
import math

import jax
import jax.numpy as jnp
import numpy as np
from jax import lax
from jax.experimental import pallas as pl
from jax.experimental.pallas import tpu as pltpu
from jax.sharding import PartitionSpec as P

WALK = 32
LANES = 128
TILE = 16
RADIX = 4


def rotation(rows, pulses, length):
    phases = (np.asarray(rows)[..., None] * np.arange(pulses)) % length
    angles = phases * (2.0 * math.pi / length)
    return np.cos(angles).astype(np.float32), np.sin(angles).astype(np.float32)


def quarter_sums(x_ref, short):
    re = [x_ref[0, 0, :, q * short:(q + 1) * short].astype(jnp.float32) for q in range(RADIX)]
    im = [x_ref[0, 1, :, q * short:(q + 1) * short].astype(jnp.float32) for q in range(RADIX)]
    are, aim, bre, bim = re[0] + re[2], im[0] + im[2], re[0] - re[2], im[0] - im[2]
    cre, cim, dre, dim = re[1] + re[3], im[1] + im[3], re[1] - re[3], im[1] - im[3]
    return (
        (are + cre, aim + cim),
        (bre + dim, bim - dre),
        (are - cre, aim - cim),
        (bre - dim, bim + dre),
    )


def power_kernel(
    batch_count, total_batches, per_band, scale,
    order_ref, x_ref, walk_ref, base_cos, base_sin, band_cos, band_sin,
    own_ref, rim_ref, table, packed, own_sum, rim_sum,
):
    step = pl.program_id(0)
    short = x_ref.shape[3] // RADIX
    bins = table.shape[1]

    @pl.when(step == 0)
    def _():
        own_sum[...] = jnp.zeros_like(own_sum)
        rim_sum[...] = jnp.zeros_like(rim_sum)
        row = lax.broadcasted_iota(jnp.int32, (TILE, short), 0) // min(per_band, TILE)

        @pl.loop(0, bins // TILE)
        def _(tile):
            start = pl.multiple_of(tile * TILE, TILE)
            first = start // per_band
            inside = pl.multiple_of(start % per_band, TILE) if per_band > TILE else 0
            vc = band_cos[pl.ds(order_ref[first], 1), :]
            vs = band_sin[pl.ds(order_ref[first], 1), :]
            for extra in range(1, max(1, TILE // per_band)):
                band = order_ref[first + extra]
                vc = jnp.where(row == extra, band_cos[pl.ds(band, 1), :], vc)
                vs = jnp.where(row == extra, band_sin[pl.ds(band, 1), :], vs)
            for r in range(RADIX):
                bc = base_cos[r, pl.ds(inside, TILE), :]
                bs = base_sin[r, pl.ds(inside, TILE), :]
                table[r, pl.ds(start, TILE), :short] = (bc * vc - bs * vs).astype(jnp.bfloat16)
                table[r, pl.ds(start, TILE), short:] = (bs * vc + bc * vs).astype(jnp.bfloat16)

    batch = lax.axis_index("slow") * batch_count + step
    lane = lax.broadcasted_iota(jnp.int32, (bins, LANES), 1)
    sums = quarter_sums(x_ref, short)
    for r in range(RADIX):
        yre, yim = (part.astype(jnp.bfloat16) for part in sums[r])
        packed[r, :LANES, :short] = yre
        packed[r, :LANES, short:] = yim
        packed[r, LANES:, :short] = yim
        packed[r, LANES:, short:] = -yre
    for r in range(RADIX):
        spec = lax.dot_general(
            table[r], packed[r], (((1,), (1,)), ((), ())), preferred_element_type=jnp.float32
        )
        re, im = spec[:, :LANES], spec[:, LANES:]
        power = re * re + im * im
        moved = walk_ref[r] * batch
        if total_batches & (total_batches - 1) == 0:
            offset = lax.shift_right_arithmetic(moved, total_batches.bit_length() - 1)
        else:
            offset = jnp.floor_divide(moved, total_batches)
        source = lane + offset
        wrapped = source & (LANES - 1)
        value = jnp.take_along_axis(power, wrapped, axis=1, mode="promise_in_bounds")
        inside = source == wrapped
        own_sum[r] += jnp.where(inside, value, 0.0)
        rim_sum[r] += jnp.where(inside, 0.0, value)

    @pl.when(step == batch_count - 1)
    def _():
        for r in range(RADIX):
            own_ref[pl.ds(r, bins, stride=RADIX), :] = own_sum[r] * scale
            rim_ref[pl.ds(r, bins, stride=RADIX), :] = rim_sum[r] * scale


def aligned_power(profiles, range_walk, band_order, total_batches):
    batch_count, _, delays, pulses = profiles.shape
    band_count = band_order.shape[0]
    band_rows = pulses // band_count
    per_band = band_rows // RADIX
    bins, short = pulses // RADIX, pulses // RADIX
    scale = 1.0 / (total_batches * pulses)
    if delays < LANES:
        profiles = jnp.pad(profiles, ((0, 0), (0, 0), (0, LANES - delays), (0, 0)))
    picked = band_order[:, None, None] == jnp.arange(band_count, dtype=jnp.int32)[None, :, None]
    walks = jnp.sum(jnp.where(picked, range_walk.reshape(1, band_count, band_rows), 0), axis=1)
    walks = jnp.broadcast_to(walks.reshape(bins, RADIX).T[:, :, None], (RADIX, bins, LANES))
    inner = np.arange(max(per_band, TILE)) % per_band
    base = rotation(RADIX * inner[None, :] + np.arange(RADIX)[:, None], short, pulses)
    band = rotation(np.arange(band_count) * band_rows, short, pulses)
    whole = lambda shape: pl.BlockSpec(shape, lambda g, order: (0,) * len(shape))
    out = jax.ShapeDtypeStruct((pulses, LANES), jnp.float32)
    return pl.pallas_call(
        functools.partial(power_kernel, batch_count, total_batches, per_band, scale),
        out_shape=(out, out),
        grid_spec=pltpu.PrefetchScalarGridSpec(
            num_scalar_prefetch=1,
            grid=(batch_count,),
            in_specs=[
                pl.BlockSpec((1, 2, LANES, pulses), lambda g, order: (g, 0, 0, 0)),
                whole(walks.shape),
                whole(base[0].shape), whole(base[1].shape),
                whole(band[0].shape), whole(band[1].shape),
            ],
            out_specs=(whole(out.shape), whole(out.shape)),
            scratch_shapes=[
                pltpu.VMEM((RADIX, bins, 2 * short), jnp.bfloat16),
                pltpu.VMEM((RADIX, 2 * LANES, 2 * short), jnp.bfloat16),
                pltpu.VMEM((RADIX, bins, LANES), jnp.float32),
                pltpu.VMEM((RADIX, bins, LANES), jnp.float32),
            ],
        ),
        compiler_params=pltpu.CompilerParams(
            dimension_semantics=("arbitrary",), vmem_limit_bytes=48 << 20
        ),
    )(band_order, profiles, walks, *(jnp.asarray(part) for part in (*base, *band)))


def neighbours(value, steps):
    count = lax.axis_size("dop")
    pairs = [(source, source + steps) for source in range(count) if 0 <= source + steps < count]
    return lax.ppermute(value, "dop", pairs)


def exchange(own, rim, delays):
    dop_count, slow_count = lax.axis_size("dop"), lax.axis_size("slow")
    rows = own.shape[0] // (dop_count * slow_count)
    after = rim[:, :WALK] if delays == LANES else own[:, delays:delays + WALK]
    from_below = neighbours(after, 1)
    from_above = neighbours(rim[:, LANES - WALK:], -1)
    own = own[:, :delays].at[:, :WALK].add(from_below)
    own = own.at[:, delays - WALK:].add(from_above)
    grouped = own.reshape(dop_count, slow_count, rows, delays)
    summed = lax.psum_scatter(grouped, "slow", scatter_dimension=1, tiled=False)
    gathered = lax.all_to_all(summed, "dop", split_axis=0, concat_axis=0, tiled=True)
    return gathered.transpose(1, 0, 2).reshape(rows, dop_count * delays)


def on_device(profiles, range_walk, band_order):
    total_batches = profiles.shape[0] * lax.axis_size("slow")
    delays = profiles.shape[2]
    own, rim = aligned_power(profiles, range_walk, band_order, total_batches)
    return exchange(own, rim, delays)


def solution(mesh):
    placed = (P("slow", None, "dop", None), P(), P())
    return jax.shard_map(
        on_device, mesh=mesh, in_specs=placed, out_specs=P(("dop", "slow"), None), check_vma=False
    )
```

```python
import functools
import math

import jax
import jax.numpy as jnp
import numpy as np
from jax import lax
from jax.experimental import pallas as pl
from jax.experimental.pallas import tpu as pltpu
from jax.sharding import PartitionSpec as P

WALK = 32
LANES = 128
TILE = 16
RADIX = 4


def rotation(rows, pulses, length):
    phases = (np.asarray(rows)[..., None] * np.arange(pulses)) % length
    angles = phases * (2.0 * math.pi / length)
    return np.cos(angles).astype(np.float32), np.sin(angles).astype(np.float32)


def quarter_sums(x_ref, short):
    re = [x_ref[0, 0, :, q * short:(q + 1) * short].astype(jnp.float32) for q in range(RADIX)]
    im = [x_ref[0, 1, :, q * short:(q + 1) * short].astype(jnp.float32) for q in range(RADIX)]
    are, aim, bre, bim = re[0] + re[2], im[0] + im[2], re[0] - re[2], im[0] - im[2]
    cre, cim, dre, dim = re[1] + re[3], im[1] + im[3], re[1] - re[3], im[1] - im[3]
    return (
        (are + cre, aim + cim),
        (bre + dim, bim - dre),
        (are - cre, aim - cim),
        (bre - dim, bim + dre),
    )


def power_kernel(
    batch_count, total_batches, per_band, scale, joined,
    order_ref, x_ref, walk_ref, turns, *refs,
):
    *outs, table, packed, own_sum, rim_sum = refs
    step = pl.program_id(0)
    short = x_ref.shape[3] // RADIX
    bins = table.shape[1]
    base_rows = max(per_band, TILE)
    bands_at = RADIX * base_rows

    @pl.when(step == 0)
    def _():
        own_sum[...] = jnp.zeros_like(own_sum)
        rim_sum[...] = jnp.zeros_like(rim_sum)
        row = lax.broadcasted_iota(jnp.int32, (TILE, short), 0) // min(per_band, TILE)

        @pl.loop(0, bins // TILE)
        def _(tile):
            start = pl.multiple_of(tile * TILE, TILE)
            first = start // per_band
            inside = pl.multiple_of(start % per_band, TILE) if per_band > TILE else 0
            vc = turns[0, pl.ds(bands_at + order_ref[first], 1), :]
            vs = turns[1, pl.ds(bands_at + order_ref[first], 1), :]
            for extra in range(1, max(1, TILE // per_band)):
                band = order_ref[first + extra]
                vc = jnp.where(row == extra, turns[0, pl.ds(bands_at + band, 1), :], vc)
                vs = jnp.where(row == extra, turns[1, pl.ds(bands_at + band, 1), :], vs)
            for r in range(RADIX):
                bc = turns[0, pl.ds(r * base_rows + inside, TILE), :]
                bs = turns[1, pl.ds(r * base_rows + inside, TILE), :]
                table[r, pl.ds(start, TILE), :short] = (bc * vc - bs * vs).astype(jnp.bfloat16)
                table[r, pl.ds(start, TILE), short:] = (bs * vc + bc * vs).astype(jnp.bfloat16)

    batch = lax.axis_index("slow") * batch_count + step
    lane = lax.broadcasted_iota(jnp.int32, (bins, LANES), 1)
    sums = quarter_sums(x_ref, short)
    for r in range(RADIX):
        yre, yim = (part.astype(jnp.bfloat16) for part in sums[r])
        packed[r, :LANES, :short] = yre
        packed[r, :LANES, short:] = yim
        packed[r, LANES:, :short] = yim
        packed[r, LANES:, short:] = -yre
    for r in range(RADIX):
        spec = lax.dot_general(
            table[r], packed[r], (((1,), (1,)), ((), ())), preferred_element_type=jnp.float32
        )
        re, im = spec[:, :LANES], spec[:, LANES:]
        power = re * re + im * im
        moved = walk_ref[r] * batch
        if total_batches & (total_batches - 1) == 0:
            offset = lax.shift_right_arithmetic(moved, total_batches.bit_length() - 1)
        else:
            offset = jnp.floor_divide(moved, total_batches)
        source = lane + offset
        wrapped = source & (LANES - 1)
        value = jnp.take_along_axis(power, wrapped, axis=1, mode="promise_in_bounds")
        inside = source == wrapped
        own_sum[r] += jnp.where(inside, value, 0.0)
        rim_sum[r] += jnp.where(inside, 0.0, value)

    @pl.when(step == batch_count - 1)
    def _():
        if joined:
            out_ref = outs[0]
            band_rows = per_band * RADIX
            half = band_rows // 2

            @pl.loop(0, bins // per_band)
            def _(block):
                rows = pl.ds(pl.multiple_of(block * per_band, per_band), per_band)
                for r in range(RADIX):
                    out_ref[block, pl.ds(r, per_band, stride=RADIX), :] = rim_sum[r, rows, :] * scale
                low, high = out_ref[block, :half, :], out_ref[block, half:band_rows, :]
                out_ref[block, band_rows:, :] = low + pltpu.roll(high, LANES // 2, 1)
                for r in range(RADIX):
                    out_ref[block, pl.ds(r, per_band, stride=RADIX), :] = own_sum[r, rows, :] * scale
        else:
            for r in range(RADIX):
                outs[0][pl.ds(r, bins, stride=RADIX), :] = own_sum[r] * scale
                outs[1][pl.ds(r, bins, stride=RADIX), :] = rim_sum[r] * scale


def aligned_power(profiles, range_walk, band_order, total_batches, joined):
    batch_count, _, delays, pulses = profiles.shape
    band_count = band_order.shape[0]
    band_rows = pulses // band_count
    per_band = band_rows // RADIX
    bins, short = pulses // RADIX, pulses // RADIX
    scale = 1.0 / (total_batches * pulses)
    if delays < LANES:
        profiles = jnp.pad(profiles, ((0, 0), (0, 0), (0, LANES - delays), (0, 0)))
    picked = band_order[:, None, None] == jnp.arange(band_count, dtype=jnp.int32)[None, :, None]
    walks = jnp.sum(jnp.where(picked, range_walk.reshape(1, band_count, band_rows), 0), axis=1)
    walks = jnp.broadcast_to(walks.reshape(bins, RADIX).T[:, :, None], (RADIX, bins, LANES))
    inner = np.arange(max(per_band, TILE)) % per_band
    base = (RADIX * inner[None, :] + np.arange(RADIX)[:, None]).reshape(-1)
    band = np.arange(band_count) * band_rows
    turns = np.stack(rotation(np.concatenate([base, band]), short, pulses))
    whole = lambda shape: pl.BlockSpec(shape, lambda g, order: (0,) * len(shape))
    if joined:
        shapes = ((band_count, band_rows + band_rows // 2, LANES),)
    else:
        shapes = ((pulses, LANES),) * 2
    return pl.pallas_call(
        functools.partial(power_kernel, batch_count, total_batches, per_band, scale, joined),
        out_shape=[jax.ShapeDtypeStruct(shape, jnp.float32) for shape in shapes],
        grid_spec=pltpu.PrefetchScalarGridSpec(
            num_scalar_prefetch=1,
            grid=(batch_count,),
            in_specs=[
                pl.BlockSpec((1, 2, LANES, pulses), lambda g, order: (g, 0, 0, 0)),
                whole(walks.shape),
                whole(turns.shape),
            ],
            out_specs=[whole(shape) for shape in shapes],
            scratch_shapes=[
                pltpu.VMEM((RADIX, bins, 2 * short), jnp.bfloat16),
                pltpu.VMEM((RADIX, 2 * LANES, 2 * short), jnp.bfloat16),
                pltpu.VMEM((RADIX, bins, LANES), jnp.float32),
                pltpu.VMEM((RADIX, bins, LANES), jnp.float32),
            ],
        ),
        compiler_params=pltpu.CompilerParams(
            dimension_semantics=("arbitrary",), vmem_limit_bytes=48 << 20
        ),
    )(band_order, profiles, walks, jnp.asarray(turns))


MESH = pl.DeviceIdType.MESH


def bit_of(value, k):
    return lax.rem(lax.div(value, 1 << k), 2)


def flipped(value, mask):
    result = value
    for k in range(mask.bit_length()):
        if mask >> k & 1:
            result = result + (1 << k) * (1 - 2 * bit_of(value, k))
    return result


def regroup_kernel(dop_count, slow_count, data, out_ref, *refs):
    levels = slow_count.bit_length() - 1
    kept, arrived = refs[:levels], refs[levels:2 * levels]
    landed, send_sem, recv_sem = refs[2 * levels:]
    dop, slow = lax.axis_index("dop"), lax.axis_index("slow")
    band_rows = out_ref.shape[0]
    partners = [(dop, flipped(slow, 1 << k)) for k in range(levels)]
    partners += [(flipped(dop, j), slow) for j in range(1, dop_count)]

    barrier = pltpu.get_barrier_semaphore()
    for partner in partners:
        pl.semaphore_signal(barrier, inc=1, device_id=partner, device_id_type=MESH)
    pl.semaphore_wait(barrier, len(partners))

    order = list(range(dop_count - 1, -1, -1))
    copies = {}

    def send(level, j, source, target, device):
        copies[level, j] = pltpu.make_async_remote_copy(
            src_ref=source, dst_ref=target,
            send_sem=send_sem.at[level, j], recv_sem=recv_sem.at[level, j],
            device_id=device, device_id_type=MESH,
        )
        copies[level, j].start()

    for j in order:
        send(0, j, data.at[flipped(dop, j), :, 1 - bit_of(slow, 0)], arrived[0].at[j], partners[0])
    for level in range(levels):
        for j in order:
            copies[level, j].wait_recv()
            bit = bit_of(slow, level)
            held = data[flipped(dop, j), :, bit] if level == 0 else kept[level - 1][j, :, bit]
            total = held + arrived[level][j]
            if level < levels - 1:
                kept[level][j] = total.reshape(kept[level].shape[1:])
                send(
                    level + 1, j, kept[level].at[j, :, 1 - bit_of(slow, level + 1)],
                    arrived[level + 1].at[j], partners[level + 1],
                )
            elif j:
                kept[level][j] = total[0]
                send(levels, j, kept[level].at[j], landed.at[j], (flipped(dop, j), slow))
            else:
                landed[0] = total[0]
    for j in order[:-1]:
        copies[levels, j].wait_recv()

    half = band_rows // 2
    lane = lax.broadcasted_iota(jnp.int32, (half, LANES), 1)
    for e in range(dop_count):
        main = landed[flipped(dop, e), :band_rows, :]
        low = jnp.zeros((half, LANES), jnp.float32)
        high = low
        for source, mine in ((e - 1, lane < WALK), (e + 1, lane >= LANES - WALK)):
            if 0 <= source < dop_count:
                rim = landed[flipped(dop, source), band_rows:, :]
                low += jnp.where(mine, rim, 0.0)
                high += jnp.where(mine, pltpu.roll(rim, LANES // 2, 1), 0.0)
        out_ref[:half, e * LANES:(e + 1) * LANES] = main[:half] + low
        out_ref[half:, e * LANES:(e + 1) * LANES] = main[half:] + high
    for copy in copies.values():
        copy.wait_send()


def regroup(blocks, dop_count, slow_count):
    rows = blocks.shape[1]
    band_rows = rows // 3 * 2
    levels = slow_count.bit_length() - 1
    kept, arrived = [], []
    count = slow_count
    for level in range(levels):
        count //= 2
        pair = (count // 2, 2) if count > 1 else ()
        kept.append(pltpu.VMEM((dop_count, *pair, rows, LANES), jnp.float32))
        arrived.append(pltpu.VMEM((dop_count, count, rows, LANES), jnp.float32))
    return pl.pallas_call(
        functools.partial(regroup_kernel, dop_count, slow_count),
        out_shape=jax.ShapeDtypeStruct((band_rows, dop_count * LANES), jnp.float32),
        in_specs=[pl.BlockSpec(memory_space=pltpu.VMEM)],
        out_specs=pl.BlockSpec(memory_space=pltpu.VMEM),
        scratch_shapes=[
            *kept, *arrived,
            pltpu.VMEM((dop_count, rows, LANES), jnp.float32),
            pltpu.SemaphoreType.DMA((levels + 1, dop_count)),
            pltpu.SemaphoreType.DMA((levels + 1, dop_count)),
        ],
        compiler_params=pltpu.CompilerParams(
            collective_id=0, has_side_effects=True, vmem_limit_bytes=32 << 20
        ),
    )(blocks.reshape(dop_count, slow_count // 2, 2, rows, LANES))


def power_of_two(count):
    return count & (count - 1) == 0


def neighbours(value, steps):
    count = lax.axis_size("dop")
    pairs = [(source, source + steps) for source in range(count) if 0 <= source + steps < count]
    return lax.ppermute(value, "dop", pairs)


def exchange(own, rim, delays):
    dop_count, slow_count = lax.axis_size("dop"), lax.axis_size("slow")
    rows = own.shape[0] // (dop_count * slow_count)
    after = rim[:, :WALK] if delays == LANES else own[:, delays:delays + WALK]
    from_below = neighbours(after, 1)
    from_above = neighbours(rim[:, LANES - WALK:], -1)
    own = own[:, :delays].at[:, :WALK].add(from_below)
    own = own.at[:, delays - WALK:].add(from_above)
    grouped = own.reshape(dop_count, slow_count, rows, delays)
    summed = lax.psum_scatter(grouped, "slow", scatter_dimension=1, tiled=False)
    gathered = lax.all_to_all(summed, "dop", split_axis=0, concat_axis=0, tiled=True)
    return gathered.transpose(1, 0, 2).reshape(rows, dop_count * delays)


def on_device(profiles, range_walk, band_order):
    total_batches = profiles.shape[0] * lax.axis_size("slow")
    delays = profiles.shape[2]
    dop_count, slow_count = lax.axis_size("dop"), lax.axis_size("slow")
    per_band = profiles.shape[3] // (dop_count * slow_count * RADIX)
    joined = (
        delays == LANES and per_band % TILE == 0 and slow_count > 1
        and power_of_two(dop_count) and power_of_two(slow_count)
    )
    sums = aligned_power(profiles, range_walk, band_order, total_batches, joined)
    if joined:
        return regroup(sums[0], dop_count, slow_count)
    return exchange(*sums, delays)


def solution(mesh):
    placed = (P("slow", None, "dop", None), P(), P())
    return jax.shard_map(
        on_device, mesh=mesh, in_specs=placed, out_specs=P(("dop", "slow"), None), check_vma=False
    )
```

```python
import functools
import math

import jax
import jax.numpy as jnp
import numpy as np
from jax import lax
from jax.experimental import pallas as pl
from jax.experimental.pallas import tpu as pltpu
from jax.sharding import PartitionSpec as P

WALK = 32
LANES = 128
TILE = 16
RADIX = 4


def rotation(rows, pulses, length):
    phases = (np.asarray(rows)[..., None] * np.arange(pulses)) % length
    angles = phases * (2.0 * math.pi / length)
    return np.cos(angles).astype(np.float32), np.sin(angles).astype(np.float32)


def quarter_sums(x_ref, at, short):
    re = [x_ref[at, 0, :, q * short:(q + 1) * short].astype(jnp.float32) for q in range(RADIX)]
    im = [x_ref[at, 1, :, q * short:(q + 1) * short].astype(jnp.float32) for q in range(RADIX)]
    are, aim, bre, bim = re[0] + re[2], im[0] + im[2], re[0] - re[2], im[0] - im[2]
    cre, cim, dre, dim = re[1] + re[3], im[1] + im[3], re[1] - re[3], im[1] - im[3]
    return (
        (are + cre, aim + cim),
        (bre + dim, bim - dre),
        (are - cre, aim - cim),
        (bre - dim, bim + dre),
    )


def power_kernel(
    batch_count, total_batches, per_band, scale, joined,
    order_ref, x_ref, walk_ref, turns, *refs,
):
    *outs, table, packed, own_sum, rim_sum, walks = refs
    step = pl.program_id(0)
    short = x_ref.shape[3] // RADIX
    bins = table.shape[1]
    base_rows = max(per_band, TILE)
    bands_at = RADIX * base_rows

    @pl.when(step == 0)
    def _():
        own_sum[...] = jnp.zeros_like(own_sum)
        rim_sum[...] = jnp.zeros_like(rim_sum)
        row = lax.broadcasted_iota(jnp.int32, (TILE, short), 0) // min(per_band, TILE)

        @pl.loop(0, bins // TILE)
        def _(tile):
            start = pl.multiple_of(tile * TILE, TILE)
            first = start // per_band
            inside = pl.multiple_of(start % per_band, TILE) if per_band > TILE else 0
            vc = turns[0, pl.ds(bands_at + order_ref[first], 1), :]
            vs = turns[1, pl.ds(bands_at + order_ref[first], 1), :]
            for extra in range(1, max(1, TILE // per_band)):
                band = order_ref[first + extra]
                vc = jnp.where(row == extra, turns[0, pl.ds(bands_at + band, 1), :], vc)
                vs = jnp.where(row == extra, turns[1, pl.ds(bands_at + band, 1), :], vs)
            for r in range(RADIX):
                if joined:
                    at = order_ref[first] * (per_band * RADIX) + inside * RADIX + r
                    walks[r, pl.ds(start, TILE), :] = walk_ref[pl.ds(at, TILE, stride=RADIX), :]
                else:
                    walks[r, pl.ds(start, TILE), :] = walk_ref[r, pl.ds(start, TILE), :]
                bc = turns[0, pl.ds(r * base_rows + inside, TILE), :]
                bs = turns[1, pl.ds(r * base_rows + inside, TILE), :]
                table[r, pl.ds(start, TILE), :short] = (bc * vc - bs * vs).astype(jnp.bfloat16)
                table[r, pl.ds(start, TILE), short:] = (bs * vc + bc * vs).astype(jnp.bfloat16)

    each = x_ref.shape[0]
    batch = lax.axis_index("slow") * batch_count + step * each
    lane = lax.broadcasted_iota(jnp.int32, (bins, LANES), 1)
    for at in range(each):
        top, low = 2 * LANES * at, 2 * LANES * at + LANES
        for r, parts in enumerate(quarter_sums(x_ref, at, short)):
            yre, yim = (part.astype(jnp.bfloat16) for part in parts)
            packed[r, top:low, :short] = yre
            packed[r, top:low, short:] = yim
            packed[r, low:low + LANES, :short] = yim
            packed[r, low:low + LANES, short:] = -yre

    def align(r, spec):
        own_add, rim_add = 0.0, 0.0
        for at in range(each):
            re = spec[:, 2 * LANES * at:2 * LANES * at + LANES]
            im = spec[:, 2 * LANES * at + LANES:2 * LANES * (at + 1)]
            power = re * re + im * im
            moved = walks[r] * (batch + at)
            if power_of_two(total_batches):
                offset = lax.shift_right_arithmetic(moved, total_batches.bit_length() - 1)
            else:
                offset = jnp.floor_divide(moved, total_batches)
            source = lane + offset
            wrapped = source & (LANES - 1)
            value = jnp.take_along_axis(power, wrapped, axis=1, mode="promise_in_bounds")
            inside = source == wrapped
            own_add += jnp.where(inside, value, 0.0)
            rim_add += jnp.where(inside, 0.0, value)
        own_sum[r] += own_add
        rim_sum[r] += rim_add

    pending = None
    for r in range(RADIX):
        spec = lax.dot_general(
            table[r], packed[r], (((1,), (1,)), ((), ())), preferred_element_type=jnp.float32
        )
        if pending is not None:
            align(r - 1, pending)
        pending = spec
    align(RADIX - 1, pending)

    @pl.when(step == pl.num_programs(0) - 1)
    def _():
        if joined:
            out_ref = outs[0]
            band_rows = per_band * RADIX
            half = band_rows // 2

            @pl.loop(0, bins // per_band)
            def _(block):
                rows = pl.ds(pl.multiple_of(block * per_band, per_band), per_band)
                for r in range(RADIX):
                    out_ref[block, pl.ds(r, per_band, stride=RADIX), :] = rim_sum[r, rows, :] * scale
                low, high = out_ref[block, :half, :], out_ref[block, half:band_rows, :]
                out_ref[block, band_rows:, :] = low + pltpu.roll(high, LANES // 2, 1)
                for r in range(RADIX):
                    out_ref[block, pl.ds(r, per_band, stride=RADIX), :] = own_sum[r, rows, :] * scale
        else:
            for r in range(RADIX):
                outs[0][pl.ds(r, bins, stride=RADIX), :] = own_sum[r] * scale
                outs[1][pl.ds(r, bins, stride=RADIX), :] = rim_sum[r] * scale


def aligned_power(profiles, range_walk, band_order, total_batches, joined):
    batch_count, _, delays, pulses = profiles.shape
    band_count = band_order.shape[0]
    band_rows = pulses // band_count
    per_band = band_rows // RADIX
    bins, short = pulses // RADIX, pulses // RADIX
    scale = 1.0 / (total_batches * pulses)
    if delays < LANES:
        profiles = jnp.pad(profiles, ((0, 0), (0, 0), (0, LANES - delays), (0, 0)))
    if joined:
        walks = jnp.broadcast_to(range_walk[:, None], (pulses, LANES))
    else:
        picked = band_order[:, None, None] == jnp.arange(band_count, dtype=jnp.int32)[None, :, None]
        walks = jnp.sum(jnp.where(picked, range_walk.reshape(1, band_count, band_rows), 0), axis=1)
        walks = jnp.broadcast_to(walks.reshape(bins, RADIX).T[:, :, None], (RADIX, bins, LANES))
    each = 2 if batch_count % 2 == 0 else 1
    inner = np.arange(max(per_band, TILE)) % per_band
    base = (RADIX * inner[None, :] + np.arange(RADIX)[:, None]).reshape(-1)
    band = np.arange(band_count) * band_rows
    turns = np.stack(rotation(np.concatenate([base, band]), short, pulses))
    whole = lambda shape: pl.BlockSpec(shape, lambda g, order: (0,) * len(shape))
    if joined:
        shapes = ((band_count, band_rows + band_rows // 2, LANES),)
    else:
        shapes = ((pulses, LANES),) * 2
    return pl.pallas_call(
        functools.partial(power_kernel, batch_count, total_batches, per_band, scale, joined),
        out_shape=[jax.ShapeDtypeStruct(shape, jnp.float32) for shape in shapes],
        grid_spec=pltpu.PrefetchScalarGridSpec(
            num_scalar_prefetch=1,
            grid=(batch_count // each,),
            in_specs=[
                pl.BlockSpec((each, 2, LANES, pulses), lambda g, order: (g, 0, 0, 0)),
                whole(walks.shape),
                whole(turns.shape),
            ],
            out_specs=[whole(shape) for shape in shapes],
            scratch_shapes=[
                pltpu.VMEM((RADIX, bins, 2 * short), jnp.bfloat16),
                pltpu.VMEM((RADIX, 2 * LANES * each, 2 * short), jnp.bfloat16),
                pltpu.VMEM((RADIX, bins, LANES), jnp.float32),
                pltpu.VMEM((RADIX, bins, LANES), jnp.float32),
                pltpu.VMEM((RADIX, bins, LANES), jnp.int32),
            ],
        ),
        compiler_params=pltpu.CompilerParams(
            dimension_semantics=("arbitrary",), vmem_limit_bytes=48 << 20
        ),
    )(band_order, profiles, walks, jnp.asarray(turns))


MESH = pl.DeviceIdType.MESH


def bit_of(value, k):
    return lax.rem(lax.div(value, 1 << k), 2)


def flipped(value, mask):
    result = value
    for k in range(mask.bit_length()):
        if mask >> k & 1:
            result = result + (1 << k) * (1 - 2 * bit_of(value, k))
    return result


def regroup_kernel(dop_count, slow_count, data, out_ref, *refs):
    levels = slow_count.bit_length() - 1
    kept, arrived = refs[:levels], refs[levels:2 * levels]
    landed, send_sem, recv_sem = refs[2 * levels:]
    dop, slow = lax.axis_index("dop"), lax.axis_index("slow")
    band_rows = out_ref.shape[0]
    partners = [(dop, flipped(slow, 1 << k)) for k in range(levels)]
    partners += [(flipped(dop, j), slow) for j in range(1, dop_count)]

    barrier = pltpu.get_barrier_semaphore()
    for partner in partners:
        pl.semaphore_signal(barrier, inc=1, device_id=partner, device_id_type=MESH)
    pl.semaphore_wait(barrier, len(partners))

    order = list(range(dop_count - 1, -1, -1))
    copies = {}

    def send(level, j, source, target, device):
        copies[level, j] = pltpu.make_async_remote_copy(
            src_ref=source, dst_ref=target,
            send_sem=send_sem.at[level, j], recv_sem=recv_sem.at[level, j],
            device_id=device, device_id_type=MESH,
        )
        copies[level, j].start()

    for j in order:
        send(0, j, data.at[flipped(dop, j), :, 1 - bit_of(slow, 0)], arrived[0].at[j], partners[0])
    for level in range(levels):
        for j in order:
            copies[level, j].wait_recv()
            bit = bit_of(slow, level)
            held = data[flipped(dop, j), :, bit] if level == 0 else kept[level - 1][j, :, bit]
            total = held + arrived[level][j]
            if level < levels - 1:
                kept[level][j] = total.reshape(kept[level].shape[1:])
                send(
                    level + 1, j, kept[level].at[j, :, 1 - bit_of(slow, level + 1)],
                    arrived[level + 1].at[j], partners[level + 1],
                )
            elif j:
                kept[level][j] = total[0]
                send(levels, j, kept[level].at[j], landed.at[j], (flipped(dop, j), slow))
            else:
                landed[0] = total[0]
    for j in order[:-1]:
        copies[levels, j].wait_recv()

    half = band_rows // 2
    lane = lax.broadcasted_iota(jnp.int32, (half, LANES), 1)
    for e in range(dop_count):
        main = landed[flipped(dop, e), :band_rows, :]
        low = jnp.zeros((half, LANES), jnp.float32)
        high = low
        for source, mine in ((e - 1, lane < WALK), (e + 1, lane >= LANES - WALK)):
            if 0 <= source < dop_count:
                rim = landed[flipped(dop, source), band_rows:, :]
                low += jnp.where(mine, rim, 0.0)
                high += jnp.where(mine, pltpu.roll(rim, LANES // 2, 1), 0.0)
        out_ref[:half, e * LANES:(e + 1) * LANES] = main[:half] + low
        out_ref[half:, e * LANES:(e + 1) * LANES] = main[half:] + high
    for copy in copies.values():
        copy.wait_send()


def regroup(blocks, dop_count, slow_count):
    rows = blocks.shape[1]
    band_rows = rows // 3 * 2
    levels = slow_count.bit_length() - 1
    kept, arrived = [], []
    count = slow_count
    for level in range(levels):
        count //= 2
        pair = (count // 2, 2) if count > 1 else ()
        kept.append(pltpu.VMEM((dop_count, *pair, rows, LANES), jnp.float32))
        arrived.append(pltpu.VMEM((dop_count, count, rows, LANES), jnp.float32))
    return pl.pallas_call(
        functools.partial(regroup_kernel, dop_count, slow_count),
        out_shape=jax.ShapeDtypeStruct((band_rows, dop_count * LANES), jnp.float32),
        in_specs=[pl.BlockSpec(memory_space=pltpu.VMEM)],
        out_specs=pl.BlockSpec(memory_space=pltpu.VMEM),
        scratch_shapes=[
            *kept, *arrived,
            pltpu.VMEM((dop_count, rows, LANES), jnp.float32),
            pltpu.SemaphoreType.DMA((levels + 1, dop_count)),
            pltpu.SemaphoreType.DMA((levels + 1, dop_count)),
        ],
        compiler_params=pltpu.CompilerParams(
            collective_id=0, has_side_effects=True, vmem_limit_bytes=32 << 20
        ),
    )(blocks.reshape(dop_count, slow_count // 2, 2, rows, LANES))


def power_of_two(count):
    return count & (count - 1) == 0


def neighbours(value, steps):
    count = lax.axis_size("dop")
    pairs = [(source, source + steps) for source in range(count) if 0 <= source + steps < count]
    return lax.ppermute(value, "dop", pairs)


def exchange(own, rim, delays):
    dop_count, slow_count = lax.axis_size("dop"), lax.axis_size("slow")
    rows = own.shape[0] // (dop_count * slow_count)
    after = rim[:, :WALK] if delays == LANES else own[:, delays:delays + WALK]
    from_below = neighbours(after, 1)
    from_above = neighbours(rim[:, LANES - WALK:], -1)
    own = own[:, :delays].at[:, :WALK].add(from_below)
    own = own.at[:, delays - WALK:].add(from_above)
    grouped = own.reshape(dop_count, slow_count, rows, delays)
    summed = lax.psum_scatter(grouped, "slow", scatter_dimension=1, tiled=False)
    gathered = lax.all_to_all(summed, "dop", split_axis=0, concat_axis=0, tiled=True)
    return gathered.transpose(1, 0, 2).reshape(rows, dop_count * delays)


def on_device(profiles, range_walk, band_order):
    total_batches = profiles.shape[0] * lax.axis_size("slow")
    delays = profiles.shape[2]
    dop_count, slow_count = lax.axis_size("dop"), lax.axis_size("slow")
    per_band = profiles.shape[3] // (dop_count * slow_count * RADIX)
    joined = (
        delays == LANES and per_band % TILE == 0 and slow_count > 1
        and power_of_two(dop_count) and power_of_two(slow_count)
    )
    sums = aligned_power(profiles, range_walk, band_order, total_batches, joined)
    if joined:
        return regroup(sums[0], dop_count, slow_count)
    return exchange(*sums, delays)


def solution(mesh):
    placed = (P("slow", None, "dop", None), P(), P())
    return jax.shard_map(
        on_device, mesh=mesh, in_specs=placed, out_specs=P(("dop", "slow"), None), check_vma=False
    )
```

```python
import functools
import math

import jax
import jax.numpy as jnp
import numpy as np
from jax import lax
from jax.experimental import pallas as pl
from jax.experimental.pallas import tpu as pltpu
from jax.sharding import PartitionSpec as P

WALK = 32
LANES = 128
TILE = 16
RADIX = 4


def rotation(rows, pulses, length):
    phases = (np.asarray(rows)[..., None] * np.arange(pulses)) % length
    angles = phases * (2.0 * math.pi / length)
    return np.cos(angles).astype(np.float32), np.sin(angles).astype(np.float32)


def quarter_sums(x_ref, at, short):
    re = [x_ref[at, 0, :, q * short:(q + 1) * short].astype(jnp.float32) for q in range(RADIX)]
    im = [x_ref[at, 1, :, q * short:(q + 1) * short].astype(jnp.float32) for q in range(RADIX)]
    are, aim, bre, bim = re[0] + re[2], im[0] + im[2], re[0] - re[2], im[0] - im[2]
    cre, cim, dre, dim = re[1] + re[3], im[1] + im[3], re[1] - re[3], im[1] - im[3]
    return (
        (are + cre, aim + cim),
        (bre + dim, bim - dre),
        (are - cre, aim - cim),
        (bre - dim, bim + dre),
    )


def power_kernel(
    batch_count, total_batches, per_band, scale, joined,
    order_ref, x_ref, walk_ref, turns, *refs,
):
    *outs, table, packed, own_sum, rim_sum, walks = refs
    step = pl.program_id(0)
    short = x_ref.shape[3] // RADIX
    bins = table.shape[1]
    base_rows = max(per_band, TILE)
    bands_at = RADIX * base_rows

    @pl.when(step == 0)
    def _():
        own_sum[...] = jnp.zeros_like(own_sum)
        rim_sum[...] = jnp.zeros_like(rim_sum)
        row = lax.broadcasted_iota(jnp.int32, (TILE, short), 0) // min(per_band, TILE)

        @pl.loop(0, bins // TILE)
        def _(tile):
            start = pl.multiple_of(tile * TILE, TILE)
            first = start // per_band
            inside = pl.multiple_of(start % per_band, TILE) if per_band > TILE else 0
            vc = turns[0, pl.ds(bands_at + order_ref[first], 1), :]
            vs = turns[1, pl.ds(bands_at + order_ref[first], 1), :]
            for extra in range(1, max(1, TILE // per_band)):
                band = order_ref[first + extra]
                vc = jnp.where(row == extra, turns[0, pl.ds(bands_at + band, 1), :], vc)
                vs = jnp.where(row == extra, turns[1, pl.ds(bands_at + band, 1), :], vs)
            for r in range(RADIX):
                if joined:
                    at = order_ref[first] * (per_band * RADIX) + inside * RADIX + r
                    walks[r, pl.ds(start, TILE), :] = walk_ref[pl.ds(at, TILE, stride=RADIX), :]
                else:
                    walks[r, pl.ds(start, TILE), :] = walk_ref[r, pl.ds(start, TILE), :]
                bc = turns[0, pl.ds(r * base_rows + inside, TILE), :]
                bs = turns[1, pl.ds(r * base_rows + inside, TILE), :]
                table[r, pl.ds(start, TILE), :short] = (bc * vc - bs * vs).astype(jnp.bfloat16)
                table[r, pl.ds(start, TILE), short:] = (bs * vc + bc * vs).astype(jnp.bfloat16)

    each = x_ref.shape[0]
    batch = lax.axis_index("slow") * batch_count + step * each
    lane = lax.broadcasted_iota(jnp.int32, (bins, LANES), 1)
    for at in range(each):
        top, low = 2 * LANES * at, 2 * LANES * at + LANES
        for r, parts in enumerate(quarter_sums(x_ref, at, short)):
            yre, yim = (part.astype(jnp.bfloat16) for part in parts)
            packed[r, top:low, :short] = yre
            packed[r, top:low, short:] = yim
            packed[r, low:low + LANES, :short] = yim
            packed[r, low:low + LANES, short:] = -yre

    def align(r, spec):
        own_add, rim_add = 0.0, 0.0
        for at in range(each):
            re = spec[:, 2 * LANES * at:2 * LANES * at + LANES]
            im = spec[:, 2 * LANES * at + LANES:2 * LANES * (at + 1)]
            power = re * re + im * im
            moved = walks[r] * (batch + at)
            if power_of_two(total_batches):
                offset = lax.shift_right_arithmetic(moved, total_batches.bit_length() - 1)
            else:
                offset = jnp.floor_divide(moved, total_batches)
            source = lane + offset
            wrapped = source & (LANES - 1)
            value = jnp.take_along_axis(power, wrapped, axis=1, mode="promise_in_bounds")
            inside = source == wrapped
            own_add += jnp.where(inside, value, 0.0)
            rim_add += jnp.where(inside, 0.0, value)
        own_sum[r] += own_add
        rim_sum[r] += rim_add

    pending = None
    for r in range(RADIX):
        spec = lax.dot_general(
            table[r], packed[r], (((1,), (1,)), ((), ())), preferred_element_type=jnp.float32
        )
        if pending is not None:
            align(r - 1, pending)
        pending = spec
    align(RADIX - 1, pending)

    @pl.when(step == pl.num_programs(0) - 1)
    def _():
        if joined:
            out_ref = outs[0]
            band_rows = per_band * RADIX
            half = band_rows // 2

            @pl.loop(0, bins // per_band)
            def _(block):
                rows = pl.ds(pl.multiple_of(block * per_band, per_band), per_band)
                for r in range(RADIX):
                    out_ref[block, pl.ds(r, per_band, stride=RADIX), :] = rim_sum[r, rows, :] * scale
                low, high = out_ref[block, :half, :], out_ref[block, half:band_rows, :]
                out_ref[block, band_rows:, :] = low + pltpu.roll(high, LANES // 2, 1)
                for r in range(RADIX):
                    out_ref[block, pl.ds(r, per_band, stride=RADIX), :] = own_sum[r, rows, :] * scale
        else:
            for r in range(RADIX):
                outs[0][pl.ds(r, bins, stride=RADIX), :] = own_sum[r] * scale
                outs[1][pl.ds(r, bins, stride=RADIX), :] = rim_sum[r] * scale


def aligned_power(profiles, range_walk, band_order, total_batches, joined):
    batch_count, _, delays, pulses = profiles.shape
    band_count = band_order.shape[0]
    band_rows = pulses // band_count
    per_band = band_rows // RADIX
    bins, short = pulses // RADIX, pulses // RADIX
    scale = 1.0 / (total_batches * pulses)
    if delays < LANES:
        profiles = jnp.pad(profiles, ((0, 0), (0, 0), (0, LANES - delays), (0, 0)))
    if joined:
        walks = jnp.broadcast_to(range_walk[:, None], (pulses, LANES))
    else:
        picked = band_order[:, None, None] == jnp.arange(band_count, dtype=jnp.int32)[None, :, None]
        walks = jnp.sum(jnp.where(picked, range_walk.reshape(1, band_count, band_rows), 0), axis=1)
        walks = jnp.broadcast_to(walks.reshape(bins, RADIX).T[:, :, None], (RADIX, bins, LANES))
    each = 2 if batch_count % 2 == 0 else 1
    inner = np.arange(max(per_band, TILE)) % per_band
    base = (RADIX * inner[None, :] + np.arange(RADIX)[:, None]).reshape(-1)
    band = np.arange(band_count) * band_rows
    turns = np.stack(rotation(np.concatenate([base, band]), short, pulses))
    whole = lambda shape: pl.BlockSpec(shape, lambda g, order: (0,) * len(shape))
    if joined:
        shapes = ((band_count, band_rows + band_rows // 2, LANES),)
    else:
        shapes = ((pulses, LANES),) * 2
    return pl.pallas_call(
        functools.partial(power_kernel, batch_count, total_batches, per_band, scale, joined),
        out_shape=[jax.ShapeDtypeStruct(shape, jnp.float32) for shape in shapes],
        grid_spec=pltpu.PrefetchScalarGridSpec(
            num_scalar_prefetch=1,
            grid=(batch_count // each,),
            in_specs=[
                pl.BlockSpec((each, 2, LANES, pulses), lambda g, order: (g, 0, 0, 0)),
                whole(walks.shape),
                whole(turns.shape),
            ],
            out_specs=[whole(shape) for shape in shapes],
            scratch_shapes=[
                pltpu.VMEM((RADIX, bins, 2 * short), jnp.bfloat16),
                pltpu.VMEM((RADIX, 2 * LANES * each, 2 * short), jnp.bfloat16),
                pltpu.VMEM((RADIX, bins, LANES), jnp.float32),
                pltpu.VMEM((RADIX, bins, LANES), jnp.float32),
                pltpu.VMEM((RADIX, bins, LANES), jnp.int32),
            ],
        ),
        compiler_params=pltpu.CompilerParams(
            dimension_semantics=("arbitrary",), vmem_limit_bytes=60 << 20
        ),
    )(band_order, profiles, walks, jnp.asarray(turns))


MESH = pl.DeviceIdType.MESH


def bit_of(value, k):
    return lax.rem(lax.div(value, 1 << k), 2)


def flipped(value, mask):
    result = value
    for k in range(mask.bit_length()):
        if mask >> k & 1:
            result = result + (1 << k) * (1 - 2 * bit_of(value, k))
    return result


def regroup_kernel(dop_count, slow_count, data, out_ref, *refs):
    levels = slow_count.bit_length() - 1
    kept, arrived = refs[:levels], refs[levels:2 * levels]
    landed, send_sem, recv_sem = refs[2 * levels:]
    dop, slow = lax.axis_index("dop"), lax.axis_index("slow")
    band_rows = out_ref.shape[0]
    partners = [(dop, flipped(slow, 1 << k)) for k in range(levels)]
    partners += [(flipped(dop, j), slow) for j in range(1, dop_count)]

    barrier = pltpu.get_barrier_semaphore()
    for partner in partners:
        pl.semaphore_signal(barrier, inc=1, device_id=partner, device_id_type=MESH)
    pl.semaphore_wait(barrier, len(partners))

    order = list(range(dop_count - 1, -1, -1))
    copies = {}

    def send(level, j, source, target, device):
        copies[level, j] = pltpu.make_async_remote_copy(
            src_ref=source, dst_ref=target,
            send_sem=send_sem.at[level, j], recv_sem=recv_sem.at[level, j],
            device_id=device, device_id_type=MESH,
        )
        copies[level, j].start()

    for j in order:
        send(0, j, data.at[flipped(dop, j), :, 1 - bit_of(slow, 0)], arrived[0].at[j], partners[0])
    for level in range(levels):
        for j in order:
            copies[level, j].wait_recv()
            bit = bit_of(slow, level)
            held = data[flipped(dop, j), :, bit] if level == 0 else kept[level - 1][j, :, bit]
            total = held + arrived[level][j]
            if level < levels - 1:
                kept[level][j] = total.reshape(kept[level].shape[1:])
                send(
                    level + 1, j, kept[level].at[j, :, 1 - bit_of(slow, level + 1)],
                    arrived[level + 1].at[j], partners[level + 1],
                )
            elif j:
                kept[level][j] = total[0]
                send(levels, j, kept[level].at[j], landed.at[j], (flipped(dop, j), slow))
            else:
                landed[0] = total[0]
    for j in order[:-1]:
        copies[levels, j].wait_recv()

    half = band_rows // 2
    lane = lax.broadcasted_iota(jnp.int32, (half, LANES), 1)
    for e in range(dop_count):
        main = landed[flipped(dop, e), :band_rows, :]
        low = jnp.zeros((half, LANES), jnp.float32)
        high = low
        for source, mine in ((e - 1, lane < WALK), (e + 1, lane >= LANES - WALK)):
            if 0 <= source < dop_count:
                rim = landed[flipped(dop, source), band_rows:, :]
                low += jnp.where(mine, rim, 0.0)
                high += jnp.where(mine, pltpu.roll(rim, LANES // 2, 1), 0.0)
        out_ref[:half, e * LANES:(e + 1) * LANES] = main[:half] + low
        out_ref[half:, e * LANES:(e + 1) * LANES] = main[half:] + high
    for copy in copies.values():
        copy.wait_send()


def regroup(blocks, dop_count, slow_count):
    rows = blocks.shape[1]
    band_rows = rows // 3 * 2
    levels = slow_count.bit_length() - 1
    kept, arrived = [], []
    count = slow_count
    for level in range(levels):
        count //= 2
        pair = (count // 2, 2) if count > 1 else ()
        kept.append(pltpu.VMEM((dop_count, *pair, rows, LANES), jnp.float32))
        arrived.append(pltpu.VMEM((dop_count, count, rows, LANES), jnp.float32))
    return pl.pallas_call(
        functools.partial(regroup_kernel, dop_count, slow_count),
        out_shape=jax.ShapeDtypeStruct((band_rows, dop_count * LANES), jnp.float32),
        in_specs=[pl.BlockSpec(memory_space=pltpu.VMEM)],
        out_specs=pl.BlockSpec(memory_space=pltpu.VMEM),
        scratch_shapes=[
            *kept, *arrived,
            pltpu.VMEM((dop_count, rows, LANES), jnp.float32),
            pltpu.SemaphoreType.DMA((levels + 1, dop_count)),
            pltpu.SemaphoreType.DMA((levels + 1, dop_count)),
        ],
        compiler_params=pltpu.CompilerParams(
            collective_id=0, has_side_effects=True, vmem_limit_bytes=32 << 20
        ),
    )(blocks.reshape(dop_count, slow_count // 2, 2, rows, LANES))


def power_of_two(count):
    return count & (count - 1) == 0


def neighbours(value, steps):
    count = lax.axis_size("dop")
    pairs = [(source, source + steps) for source in range(count) if 0 <= source + steps < count]
    return lax.ppermute(value, "dop", pairs)


def exchange(own, rim, delays):
    dop_count, slow_count = lax.axis_size("dop"), lax.axis_size("slow")
    rows = own.shape[0] // (dop_count * slow_count)
    after = rim[:, :WALK] if delays == LANES else own[:, delays:delays + WALK]
    from_below = neighbours(after, 1)
    from_above = neighbours(rim[:, LANES - WALK:], -1)
    own = own[:, :delays].at[:, :WALK].add(from_below)
    own = own.at[:, delays - WALK:].add(from_above)
    grouped = own.reshape(dop_count, slow_count, rows, delays)
    summed = lax.psum_scatter(grouped, "slow", scatter_dimension=1, tiled=False)
    gathered = lax.all_to_all(summed, "dop", split_axis=0, concat_axis=0, tiled=True)
    return gathered.transpose(1, 0, 2).reshape(rows, dop_count * delays)


def on_device(profiles, range_walk, band_order):
    total_batches = profiles.shape[0] * lax.axis_size("slow")
    delays = profiles.shape[2]
    dop_count, slow_count = lax.axis_size("dop"), lax.axis_size("slow")
    per_band = profiles.shape[3] // (dop_count * slow_count * RADIX)
    joined = (
        delays == LANES and per_band % TILE == 0 and slow_count > 1
        and power_of_two(dop_count) and power_of_two(slow_count)
    )
    sums = aligned_power(profiles, range_walk, band_order, total_batches, joined)
    if joined:
        return regroup(sums[0], dop_count, slow_count)
    return exchange(*sums, delays)


def solution(mesh):
    placed = (P("slow", None, "dop", None), P(), P())
    return jax.shard_map(
        on_device, mesh=mesh, in_specs=placed, out_specs=P(("dop", "slow"), None), check_vma=False
    )
```
